32 devices in a mesh: rep: 2 (over x), tp: 4 (over z), sp: 4 (over y, core).
Axes of the slice: x: 2, y: 2, z: 4, core: 2. Of those that a mesh axis runs over, the one named last changes fastest.
Arguments:
- x: bfloat16 [8192, 5376], P(('rep', 'sp')), parts along dimension 0
- pos: int32 [8192], P(('rep', 'sp')), parts along dimension 0
- g1: float32 [5376], replicated
- g2: float32 [5376], replicated
- wq: bfloat16 [5376, 4096], P(None, 'tp')
- wk: bfloat16 [5376, 2048], P(None, 'tp')
- wv: bfloat16 [5376, 2048], P(None, 'tp')
- wo: bfloat16 [4096, 5376], P('tp')
- w1: bfloat16 [5376, 21504], P(None, 'tp')
- w3: bfloat16 [5376, 21504], P(None, 'tp')
- w2: bfloat16 [21504, 5376], P('tp')
Outputs:
- output 1: bfloat16 [8192, 5376], P(('rep', 'sp')), parts along dimension 0
- output 2: bfloat16 [8192, 16, 128], P('rep', ('tp', 'sp')), parts along dimension 0
- output 3: bfloat16 [8192, 16, 128], P('rep', ('tp', 'sp')), parts along dimension 0
There are 2 independent parts. The reference program is written for one: setup_inputs(seed, part) draws one part's arguments, and reference() takes and returns one part's arrays. A program takes and returns all parts, laid end to end along the dimension named above; an argument that names none is the same for every part.
All inputs are finite; a program needn't handle non-finite values.
Results may differ from the reference program's by a relative error of at most 0.00743013.
Values are sent between devices in bfloat16 or wider.
A program may use at most 1 GiB of HBM per device.

```python
import jax
import jax.numpy as jnp
from jax import lax

TOKENS = 4096
D = 5376
FF = 21504
HEADS = 32
KV_HEADS = 16
HEAD_DIM = 128
KV_REP = 16

EPS = 1e-5
ROPE_BASE = 5e5
NEG = -1e30
SCALE = HEAD_DIM ** -0.5
QBLOCK = min(512, TOKENS)
GROUP = HEADS // KV_HEADS


def setup_inputs(seed: int = 0, part: int = 0) -> dict:
    key = jax.random.PRNGKey(seed)
    ks = jax.random.split(key, 10)
    kx, kp = jax.random.split(jax.random.fold_in(ks[9], part))

    def w(k, shape, fan_in, gain=1.0):
        return (jax.random.normal(k, shape, jnp.float32) * (gain * fan_in ** -0.5)).astype(jnp.bfloat16)

    return {
        "x": jax.random.normal(kx, (TOKENS, D), jnp.float32).astype(jnp.bfloat16),
        "pos": jnp.arange(TOKENS, dtype=jnp.int32) + jax.random.randint(kp, (), 0, 8192, jnp.int32),
        "g1": 1.0 + 0.1 * jax.random.normal(ks[0], (D,), jnp.float32),
        "g2": 1.0 + 0.1 * jax.random.normal(ks[1], (D,), jnp.float32),
        "wq": w(ks[2], (D, HEADS * HEAD_DIM), D, 1.4),
        "wk": w(ks[3], (D, KV_HEADS * HEAD_DIM), D, 1.4),
        "wv": w(ks[4], (D, KV_HEADS * HEAD_DIM), D),
        "wo": w(ks[5], (HEADS * HEAD_DIM, D), HEADS * HEAD_DIM),
        "w1": w(ks[6], (D, FF), D),
        "w3": w(ks[7], (D, FF), D),
        "w2": w(ks[8], (FF, D), FF),
    }


def _rms(x, g):
    x32 = x.astype(jnp.float32)
    r = lax.rsqrt(jnp.mean(x32 * x32, axis=-1, keepdims=True) + EPS)
    return (x32 * r * g).astype(jnp.bfloat16)


def _rope(t, pos):
    half = HEAD_DIM // 2
    inv = ROPE_BASE ** (-2.0 * jnp.arange(half, dtype=jnp.float32) / HEAD_DIM)
    ang = pos.astype(jnp.float32)[:, None] * inv[None, :]
    c = jnp.cos(ang)[:, None, :]
    s = jnp.sin(ang)[:, None, :]
    t1, t2 = t[..., :half], t[..., half:]
    return jnp.concatenate([t1 * c - t2 * s, t2 * c + t1 * s], axis=-1)


def _attend(q, k, v):
    nb = TOKENS // QBLOCK
    qh = q.reshape(nb, QBLOCK, KV_HEADS, GROUP, HEAD_DIM).transpose(2, 0, 3, 1, 4)
    kh = k.transpose(1, 0, 2)
    vh = v.transpose(1, 0, 2)
    cols = jnp.arange(TOKENS)

    def head(a):
        qq, kk, vv = a
        kk = kk.astype(jnp.float32)
        vv = vv.astype(jnp.float32)

        def block(b):
            qb, i = b
            s = jnp.einsum("gqd,nd->gqn", qb.astype(jnp.float32), kk) * SCALE
            rows = i * QBLOCK + jnp.arange(QBLOCK)
            s = jnp.where(rows[:, None] >= cols[None, :], s, NEG)
            p = jax.nn.softmax(s, axis=-1).astype(jnp.bfloat16)
            return jnp.einsum("gqn,nd->gqd", p.astype(jnp.float32), vv).astype(jnp.bfloat16)

        return lax.map(block, (qq, jnp.arange(nb)))

    o = lax.map(head, (qh, kh, vh))
    return o.transpose(1, 3, 0, 2, 4).reshape(TOKENS, HEADS * HEAD_DIM)


def _mlp(x1, g2, w1, w3, w2):
    nb = TOKENS // QBLOCK

    def block(xb):
        u2 = _rms(xb, g2)
        a = jnp.dot(u2, w1, preferred_element_type=jnp.float32)
        b = jnp.dot(u2, w3, preferred_element_type=jnp.float32)
        hid = (jax.nn.silu(a) * b).astype(jnp.bfloat16)
        return (xb.astype(jnp.float32) + jnp.dot(hid, w2, preferred_element_type=jnp.float32)).astype(jnp.bfloat16)

    return lax.map(block, x1.reshape(nb, QBLOCK, D)).reshape(TOKENS, D)


def reference(x, pos, g1, g2, wq, wk, wv, wo, w1, w3, w2):
    u = _rms(x, g1)
    q = _rope(jnp.dot(u, wq, preferred_element_type=jnp.float32).reshape(TOKENS, HEADS, HEAD_DIM), pos).astype(jnp.bfloat16)
    k = _rope(jnp.dot(u, wk, preferred_element_type=jnp.float32).reshape(TOKENS, KV_HEADS, HEAD_DIM), pos).astype(jnp.bfloat16)
    v = jnp.dot(u, wv, preferred_element_type=jnp.float32).astype(jnp.bfloat16).reshape(TOKENS, KV_HEADS, HEAD_DIM)
    a = _attend(q, k, v)
    x1 = (x.astype(jnp.float32) + jnp.dot(a, wo, preferred_element_type=jnp.float32)).astype(jnp.bfloat16)
    y = _mlp(x1, g2, w1, w3, w2)
    r = KV_REP // KV_HEADS
    return y, jnp.repeat(k, r, axis=1), jnp.repeat(v, r, axis=1)
```

```python
import functools

import jax
import jax.numpy as jnp
from jax import lax
from jax.experimental import pallas as pl
from jax.experimental.pallas import tpu as pltpu
from jax.sharding import PartitionSpec as P

HEAD_DIM = 128
EPS = 1e-5
ROPE_BASE = 5e5
NEG = -1e30
QB = 512
KB = 512
TILE = 128
LAG = 2
RING = 3 * LAG + 2
MROWS = 256
MESH = pl.DeviceIdType.MESH


def _rms(x, g):
    x32 = x.astype(jnp.float32)
    r = lax.rsqrt(jnp.mean(x32 * x32, axis=-1, keepdims=True) + EPS)
    return (x32 * r * g).astype(jnp.bfloat16)


def _angles(pos):
    half = HEAD_DIM // 2
    inv = ROPE_BASE ** (-2.0 * jnp.arange(half, dtype=jnp.float32) / HEAD_DIM)
    ang = pos.astype(jnp.float32)[..., None] * inv
    return jnp.cos(ang)[..., None, :], jnp.sin(ang)[..., None, :]


def _rope(t, cs):
    c, s = cs
    half = HEAD_DIM // 2
    t1, t2 = t[..., :half], t[..., half:]
    return jnp.concatenate([t1 * c - t2 * s, t2 * c + t1 * s], axis=-1)


def _attn_kernel(q_ref, k_ref, v_ref, o_ref, *, heads, per_src):
    i = pl.program_id(0)
    scale = HEAD_DIM ** -0.5
    q = q_ref[0].reshape(heads * QB, HEAD_DIM)
    rows = heads * QB

    def scores(j):
        kb = k_ref[j // per_src, 0, pl.ds((j % per_src) * KB, KB), :]
        return lax.dot_general(q, kb, (((1,), (1,)), ((), ())), preferred_element_type=jnp.float32) * scale

    def update(j, s, carry):
        m, l, acc = carry
        mn = jnp.maximum(m, jnp.max(s, axis=1, keepdims=True))
        a = jnp.exp(m - mn)
        p = jnp.exp(s - mn)
        l = l * a + jnp.sum(p, axis=1, keepdims=True)
        vb = v_ref[j // per_src, 0, pl.ds((j % per_src) * KB, KB), :]
        acc = acc * a + jnp.dot(p.astype(jnp.bfloat16), vb, preferred_element_type=jnp.float32)
        return mn, l, acc

    init = (
        jnp.full((rows, 1), NEG, jnp.float32),
        jnp.zeros((rows, 1), jnp.float32),
        jnp.zeros((rows, HEAD_DIM), jnp.float32),
    )
    carry = lax.fori_loop(0, i, lambda j, c: update(j, scores(j), c), init)
    r = lax.broadcasted_iota(jnp.int32, (heads, QB, KB), 1)
    c = lax.broadcasted_iota(jnp.int32, (heads, QB, KB), 2)
    s = jnp.where((r >= c).reshape(rows, KB), scores(i), NEG)
    _, l, acc = update(i, s, carry)
    o = (acc / l).astype(jnp.bfloat16)
    for h in range(heads):
        o_ref[0, :, h * HEAD_DIM:(h + 1) * HEAD_DIM] = o[h * QB:(h + 1) * QB]


def _attention(buf, heads):
    sp, _, m, dh = buf.shape
    per = m // QB
    n = sp * m
    return pl.pallas_call(
        functools.partial(_attn_kernel, heads=heads, per_src=m // KB),
        grid=(n // QB,),
        in_specs=[
            pl.BlockSpec((1, heads, QB, dh), lambda i: (i // per, 0, i % per, 0)),
            pl.BlockSpec((sp, 1, m, dh), lambda i: (0, heads, 0, 0)),
            pl.BlockSpec((sp, 1, m, dh), lambda i: (0, heads + 1, 0, 0)),
        ],
        out_specs=pl.BlockSpec((1, QB, heads * dh), lambda i: (i // per, i % per, 0)),
        out_shape=jax.ShapeDtypeStruct((sp, m, heads * dh), jnp.bfloat16),
        cost_estimate=pl.CostEstimate(flops=4 * heads * n * n * dh, bytes_accessed=8 * n * dh * 2, transcendentals=heads * n * n // 2),
        compiler_params=pltpu.CompilerParams(vmem_limit_bytes=48 * 1024 * 1024),
        name="attn",
    )(buf, buf, buf)


def _line_gather(a, t):
    up, dn = [a], [a]
    for k in range(1, 4):
        up.append(lax.ppermute(up[-1], "tp", [(i, i + 1) for i in range(k - 1, 3)]))
        dn.append(lax.ppermute(dn[-1], "tp", [(i, i - 1) for i in range(1, 5 - k)]))
    out = []
    for s in range(4):
        b = a
        for d in range(4):
            if d < s:
                b = jnp.where(t == d, dn[s - d], b)
            elif d > s:
                b = jnp.where(t == d, up[d - s], b)
        out.append(b)
    return out


def _mlp_out_kernel(hid_ref, w2_ref, x1_ref, y_ref, acc, part, fin, sf, rf, sb, rb, sl, *, nt):
    i = pl.program_id(0)
    t = lax.axis_index("tp")
    h = part.shape[1] // 2

    @pl.when(i == 0)
    def _():
        barrier = pltpu.get_barrier_semaphore()

        @pl.when(t > 0)
        def _():
            pl.semaphore_signal(barrier, inc=1, device_id={"tp": t - 1}, device_id_type=MESH)

        @pl.when(t < 3)
        def _():
            pl.semaphore_signal(barrier, inc=1, device_id={"tp": t + 1}, device_id_type=MESH)

        pl.semaphore_wait(barrier, jnp.where((t == 0) | (t == 3), 1, 2))

    def forward(s, k, dev):
        return pltpu.make_async_remote_copy(
            src_ref=acc.at[s, k], dst_ref=acc.at[s, k], send_sem=sf.at[s, k], recv_sem=rf.at[s, k],
            device_id={"tp": dev}, device_id_type=MESH)

    def back(s, k, dev, src):
        return pltpu.make_async_remote_copy(
            src_ref=src, dst_ref=y_ref.at[s, k], send_sem=sb.at[s, k], recv_sem=rb.at[s, k],
            device_id={"tp": dev}, device_id_type=MESH)

    def keep(s, k):
        return pltpu.make_async_copy(fin.at[k], y_ref.at[s, k], sl.at[k])

    other = jnp.where(t < 2, t + 1, t - 1)
    for s in range(2):
        pos = 3 - t if s == 0 else t
        nxt = t - 1 if s == 0 else t + 1
        prv = t + 1 if s == 0 else t - 1
        rows = slice(s * h, (s + 1) * h)
        k = i - 1 - pos * LAG
        on = (k >= 0) & (k < nt)

        @pl.when(on & (pos == 0))
        def _():
            acc[s, k] = part[k % RING, rows, :]
            forward(s, k, nxt).start()

        @pl.when(on & (pos > 0) & (pos < 3))
        def _():
            forward(s, k, other).wait_recv()
            acc[s, k] = acc[s, k] + part[k % RING, rows, :]
            forward(s, k, nxt).start()

        @pl.when(on & (pos == 3))
        def _():
            forward(s, k, other).wait_recv()
            total = acc[s, k] + part[k % RING, rows, :]
            fin[k] = (x1_ref[rows, :].astype(jnp.float32) + total).astype(jnp.bfloat16)
            back(s, k, prv, fin.at[k]).start()
            keep(s, k).start()

        kb = i - 1 - 3 * LAG - (3 - pos) * LAG
        onb = (kb >= 0) & (kb < nt)

        @pl.when(onb & (pos > 0) & (pos < 3))
        def _():
            back(s, kb, other, y_ref.at[s, kb]).wait_recv()
            back(s, kb, prv, y_ref.at[s, kb]).start()

        @pl.when(onb & (pos == 0))
        def _():
            back(s, kb, other, y_ref.at[s, kb]).wait_recv()

    @pl.when(i < nt)
    def _():
        def block(b, _):
            r = pl.ds(pl.multiple_of(b * MROWS, MROWS), MROWS)
            part[i % RING, r, :] = jnp.dot(hid_ref[r, :], w2_ref[...], preferred_element_type=jnp.float32)
            return 0

        lax.fori_loop(0, part.shape[1] // MROWS, block, 0)

    @pl.when(i == nt + 6 * LAG)
    def _():
        for s in range(2):
            pos = 3 - t if s == 0 else t

            def drain(k, _):
                @pl.when(pos < 3)
                def _():
                    forward(s, k, other).wait_send()

                @pl.when(pos > 0)
                def _():
                    back(s, k, other, fin.at[k]).wait_send()

                @pl.when(pos == 3)
                def _():
                    keep(s, k).wait()

                return 0

            lax.fori_loop(0, nt, drain, 0)


def _mlp_out(hid, w2, x1):
    m, f = hid.shape
    d = w2.shape[1]
    nt = d // TILE
    y = pl.pallas_call(
        functools.partial(_mlp_out_kernel, nt=nt),
        grid=(nt + 6 * LAG + 1,),
        in_specs=[
            pl.BlockSpec((m, f), lambda i: (0, 0), pipeline_mode=pl.Buffered(1)),
            pl.BlockSpec((f, TILE), lambda i: (0, jnp.minimum(i, nt - 1))),
            pl.BlockSpec((m, TILE), lambda i: (0, jnp.clip(i - 1 - 3 * LAG, 0, nt - 1))),
        ],
        out_specs=pl.BlockSpec(memory_space=pl.ANY),
        out_shape=jax.ShapeDtypeStruct((2, nt, m // 2, TILE), jnp.bfloat16),
        scratch_shapes=[
            pltpu.VMEM((2, nt, m // 2, TILE), jnp.float32),
            pltpu.VMEM((RING, m, TILE), jnp.float32),
            pltpu.VMEM((nt, m // 2, TILE), jnp.bfloat16),
            pltpu.SemaphoreType.DMA((2, nt)),
            pltpu.SemaphoreType.DMA((2, nt)),
            pltpu.SemaphoreType.DMA((2, nt)),
            pltpu.SemaphoreType.DMA((2, nt)),
            pltpu.SemaphoreType.DMA((nt,)),
        ],
        cost_estimate=pl.CostEstimate(flops=2 * m * f * d, bytes_accessed=2 * f * d + 6 * m * d, transcendentals=0),
        compiler_params=pltpu.CompilerParams(
            collective_id=0, has_side_effects=True, vmem_limit_bytes=60 * 1024 * 1024, dimension_semantics=("arbitrary",)),
        name="mlp_out",
    )(hid, w2, x1)
    return y.transpose(0, 2, 1, 3).reshape(m, d)


def solution(mesh):
    sp = mesh.shape["sp"]
    nrep = mesh.shape["rep"]
    tok = P(("rep", "sp"), None)
    col = P(None, "tp")
    row = P("tp", None)
    cache = P("rep", ("tp", "sp"), None)

    def local(x, pos, g1, g2, wq, wk, wv, wo, w1, w3, w2):
        m, d = x.shape
        n = m * sp
        ht = wq.shape[1] // HEAD_DIM
        kt = wk.shape[1] // HEAD_DIM
        qh = ht // sp
        t = lax.axis_index("tp")
        part = wo.shape[0] // (nrep * sp)
        mine = lax.axis_index("rep") * sp + lax.axis_index("sp")
        wo_all = lax.all_gather(lax.dynamic_slice_in_dim(wo, mine * part, part, 0), ("tp", "rep", "sp"), axis=0, tiled=True)

        u = _rms(x, g1)
        cs = _angles(pos)
        q = _rope(jnp.dot(u, wq, preferred_element_type=jnp.float32).reshape(m, ht, HEAD_DIM), cs).astype(jnp.bfloat16)
        k = _rope(jnp.dot(u, wk, preferred_element_type=jnp.float32).reshape(m, kt, HEAD_DIM), cs).astype(jnp.bfloat16)
        v = jnp.dot(u, wv, preferred_element_type=jnp.float32).astype(jnp.bfloat16).reshape(m, kt, HEAD_DIM)
        buf = jnp.concatenate([q.reshape(m, sp, qh, HEAD_DIM), k.reshape(m, sp, 1, HEAD_DIM), v.reshape(m, sp, 1, HEAD_DIM)], axis=2)
        buf = lax.all_to_all(buf.transpose(1, 2, 0, 3), "sp", 0, 0, tiled=True)
        ka = buf[:, qh].reshape(n, 1, HEAD_DIM)
        va = buf[:, qh + 1].reshape(n, 1, HEAD_DIM)
        att = _attention(buf, qh)
        att = lax.all_to_all(att, "sp", 0, 0, tiled=True)
        att = att.transpose(1, 0, 2).reshape(m, ht * HEAD_DIM)
        att = jnp.concatenate(_line_gather(att, t), axis=1)

        o = jnp.dot(att, wo_all, preferred_element_type=jnp.float32)
        x1 = (x.astype(jnp.float32) + o).astype(jnp.bfloat16)
        u2 = _rms(x1, g2)
        hid = (jax.nn.silu(jnp.dot(u2, w1, preferred_element_type=jnp.float32)) * jnp.dot(u2, w3, preferred_element_type=jnp.float32)).astype(jnp.bfloat16)
        y = _mlp_out(hid, w2, x1)
        return y, ka, va

    return jax.shard_map(
        local,
        mesh=mesh,
        in_specs=(tok, P(("rep", "sp")), P(), P(), col, col, col, row, col, col, row),
        out_specs=(tok, cache, cache),
        check_vma=False,
    )
```

```python
import functools

import jax
import jax.numpy as jnp
from jax import lax
from jax.experimental import pallas as pl
from jax.experimental.pallas import tpu as pltpu
from jax.sharding import PartitionSpec as P


HEAD_DIM = 128
EPS = 1e-5
ROPE_BASE = 5e5
NEG = -1e30
QB = 512
KB = 512
TILE = 256
LAG = 2
RING = 3 * LAG + 2
MROWS = 256
MESH = pl.DeviceIdType.MESH


def _rms(x, g):
    x32 = x.astype(jnp.float32)
    r = lax.rsqrt(jnp.mean(x32 * x32, axis=-1, keepdims=True) + EPS)
    return (x32 * r * g).astype(jnp.bfloat16)


def _angles(pos):
    half = HEAD_DIM // 2
    inv = ROPE_BASE ** (-2.0 * jnp.arange(half, dtype=jnp.float32) / HEAD_DIM)
    ang = pos.astype(jnp.float32)[..., None] * inv
    return jnp.cos(ang)[..., None, :], jnp.sin(ang)[..., None, :]


def _rope(t, cs):
    c, s = cs
    half = HEAD_DIM // 2
    t1, t2 = t[..., :half], t[..., half:]
    return jnp.concatenate([t1 * c - t2 * s, t2 * c + t1 * s], axis=-1)


def _attn_kernel(q_ref, k_ref, v_ref, o_ref, *, heads, per_src):
    i = pl.program_id(0)
    scale = HEAD_DIM ** -0.5
    q = q_ref[0].reshape(heads * QB, HEAD_DIM)
    rows = heads * QB

    def scores(j):
        kb = k_ref[j // per_src, 0, pl.ds((j % per_src) * KB, KB), :]
        return lax.dot_general(q, kb, (((1,), (1,)), ((), ())), preferred_element_type=jnp.float32) * scale

    def update(j, s, carry):
        m, l, acc = carry
        mn = jnp.maximum(m, jnp.max(s, axis=1, keepdims=True))
        a = jnp.exp(m - mn)
        p = jnp.exp(s - mn)
        l = l * a + jnp.sum(p, axis=1, keepdims=True)
        vb = v_ref[j // per_src, 0, pl.ds((j % per_src) * KB, KB), :]
        acc = acc * a + jnp.dot(p.astype(jnp.bfloat16), vb, preferred_element_type=jnp.float32)
        return mn, l, acc

    init = (
        jnp.full((rows, 1), NEG, jnp.float32),
        jnp.zeros((rows, 1), jnp.float32),
        jnp.zeros((rows, HEAD_DIM), jnp.float32),
    )
    carry = lax.fori_loop(0, i, lambda j, c: update(j, scores(j), c), init)
    r = lax.broadcasted_iota(jnp.int32, (heads, QB, KB), 1)
    c = lax.broadcasted_iota(jnp.int32, (heads, QB, KB), 2)
    s = jnp.where((r >= c).reshape(rows, KB), scores(i), NEG)
    _, l, acc = update(i, s, carry)
    o = (acc / l).astype(jnp.bfloat16)
    for h in range(heads):
        o_ref[0, :, h * HEAD_DIM:(h + 1) * HEAD_DIM] = o[h * QB:(h + 1) * QB]


def _attention(buf, heads):
    sp, _, m, dh = buf.shape
    per = m // QB
    n = sp * m
    return pl.pallas_call(
        functools.partial(_attn_kernel, heads=heads, per_src=m // KB),
        grid=(n // QB,),
        in_specs=[
            pl.BlockSpec((1, heads, QB, dh), lambda i: (i // per, 0, i % per, 0)),
            pl.BlockSpec((sp, 1, m, dh), lambda i: (0, heads, 0, 0)),
            pl.BlockSpec((sp, 1, m, dh), lambda i: (0, heads + 1, 0, 0)),
        ],
        out_specs=pl.BlockSpec((1, QB, heads * dh), lambda i: (i // per, i % per, 0)),
        out_shape=jax.ShapeDtypeStruct((sp, m, heads * dh), jnp.bfloat16),
        cost_estimate=pl.CostEstimate(flops=4 * heads * n * n * dh, bytes_accessed=8 * n * dh * 2, transcendentals=heads * n * n // 2),
        compiler_params=pltpu.CompilerParams(vmem_limit_bytes=48 * 1024 * 1024),
        name="attn",
    )(buf, buf, buf)


def _hop(up, dn, k):
    up = lax.ppermute(up, "tp", [(i, i + 1) for i in range(k - 1, 3)])
    dn = lax.ppermute(dn, "tp", [(i, i - 1) for i in range(1, 5 - k)])
    return up, dn


def _side_by_side(a, up, dn, t):
    out = []
    for s in range(4):
        b = a
        for d in range(4):
            if d < s:
                b = jnp.where(t == d, dn[s - d - 1], b)
            elif d > s:
                b = jnp.where(t == d, up[d - s - 1], b)
        out.append(b)
    return jnp.concatenate(out, axis=1)


def _mlp_kernel(hid_ref, u_ref, w1_ref, w3_ref, w2_ref, x0_ref, x1_ref, y_ref, acc, part, fin, hid, sf, rf, sb, rb, sl, *, nc, nt):
    i = pl.program_id(0)
    t = lax.axis_index("tp")
    m = part.shape[1]
    h = m // 2

    @pl.when(i == 0)
    def _():
        barrier = pltpu.get_barrier_semaphore()

        @pl.when(t > 0)
        def _():
            pl.semaphore_signal(barrier, inc=1, device_id={"tp": t - 1}, device_id_type=MESH)

        @pl.when(t < 3)
        def _():
            pl.semaphore_signal(barrier, inc=1, device_id={"tp": t + 1}, device_id_type=MESH)

        pl.semaphore_wait(barrier, jnp.where((t == 0) | (t == 3), 1, 2))

    def place(s, g):
        row = pl.multiple_of((g // nc) * m + s * h, h)
        return y_ref.at[pl.ds(row, h), pl.ds(pl.multiple_of((g % nc) * TILE, TILE), TILE)]

    def forward(s, g, dev):
        return pltpu.make_async_remote_copy(
            src_ref=acc.at[s, g], dst_ref=acc.at[s, g], send_sem=sf.at[s, g], recv_sem=rf.at[s, g],
            device_id={"tp": dev}, device_id_type=MESH)

    def back(s, g, dev, src):
        return pltpu.make_async_remote_copy(
            src_ref=src, dst_ref=place(s, g), send_sem=sb.at[s, g], recv_sem=rb.at[s, g],
            device_id={"tp": dev}, device_id_type=MESH)

    def keep(s, g):
        return pltpu.make_async_copy(fin.at[g % RING], place(s, g), sl.at[g])

    def settle(s, g, dev):
        back(s, g, dev, fin.at[g % RING]).wait_send()
        keep(s, g).wait()

    other = jnp.where(t < 2, t + 1, t - 1)
    for s in range(2):
        pos = 3 - t if s == 0 else t
        nxt = t - 1 if s == 0 else t + 1
        prv = t + 1 if s == 0 else t - 1
        rows = slice(s * h, (s + 1) * h)
        g = i - 1 - pos * LAG
        on = (g >= 0) & (g < nt)

        @pl.when(on & (pos == 0))
        def _():
            acc[s, g] = part[g % RING, rows, :]
            forward(s, g, nxt).start()

        @pl.when(on & (pos > 0) & (pos < 3))
        def _():
            forward(s, g, other).wait_recv()
            acc[s, g] = acc[s, g] + part[g % RING, rows, :]
            forward(s, g, nxt).start()

        @pl.when(on & (pos == 3))
        def _():
            forward(s, g, other).wait_recv()
            total = acc[s, g] + part[g % RING, rows, :]

            @pl.when(g >= RING)
            def _():
                settle(s, g - RING, prv)

            res = jnp.where(g < nc, x0_ref[rows, :].astype(jnp.float32), x1_ref[rows, :].astype(jnp.float32))
            fin[g % RING] = (res + total).astype(jnp.bfloat16)
            back(s, g, prv, fin.at[g % RING]).start()
            keep(s, g).start()

        gb = i - 1 - 3 * LAG - (3 - pos) * LAG
        onb = (gb >= 0) & (gb < nt)

        @pl.when(onb & (pos > 0) & (pos < 3))
        def _():
            back(s, gb, other, place(s, gb)).wait_recv()
            back(s, gb, prv, place(s, gb)).start()

        @pl.when(onb & (pos == 0))
        def _():
            back(s, gb, other, place(s, gb)).wait_recv()

    def blocks(body):
        def step(b, _):
            body(pl.ds(pl.multiple_of(b * MROWS, MROWS), MROWS))
            return 0

        lax.fori_loop(0, m // MROWS, step, 0)

    @pl.when(i < nc)
    def _():
        cols = pl.ds(pl.multiple_of(i * TILE, TILE), TILE)

        def body(r):
            a = jnp.dot(u_ref[r, :], w1_ref[...], preferred_element_type=jnp.float32)
            b = jnp.dot(u_ref[r, :], w3_ref[...], preferred_element_type=jnp.float32)
            hid[r, cols] = (jax.nn.silu(a) * b).astype(jnp.bfloat16)
            part[i % RING, r, :] = jnp.dot(hid_ref[r, :], w2_ref[...], preferred_element_type=jnp.float32)

        blocks(body)

    @pl.when((i >= nc) & (i < nt))
    def _():
        def body(r):
            part[i % RING, r, :] = jnp.dot(hid[r, :], w2_ref[...], preferred_element_type=jnp.float32)

        blocks(body)

    @pl.when(i == nt + 6 * LAG)
    def _():
        for s in range(2):
            pos = 3 - t if s == 0 else t

            def drain(g, _):
                @pl.when(pos < 3)
                def _():
                    forward(s, g, other).wait_send()

                @pl.when((pos > 0) & (pos < 3))
                def _():
                    back(s, g, other, place(s, g)).wait_send()

                @pl.when((pos == 3) & (g >= nt - RING))
                def _():
                    settle(s, g, other)

                return 0

            lax.fori_loop(0, nt, drain, 0)


def _mlp_out(hid, u, w1, w3, w2, xs):
    m, f = hid.shape
    d = w2.shape[1]
    nc = d // TILE
    nt = 2 * nc
    assert f == d

    def late(i):
        return jnp.clip(i - 1 - 3 * LAG, 0, nt - 1)

    once = pl.Buffered(1)
    return pl.pallas_call(
        functools.partial(_mlp_kernel, nc=nc, nt=nt),
        grid=(nt + 6 * LAG + 1,),
        in_specs=[
            pl.BlockSpec((m, f), lambda i: (0, 0), pipeline_mode=once),
            pl.BlockSpec((m, u.shape[1]), lambda i: (0, 0), pipeline_mode=once),
            pl.BlockSpec((w1.shape[0], TILE), lambda i: (0, jnp.minimum(i, nc - 1))),
            pl.BlockSpec((w3.shape[0], TILE), lambda i: (0, jnp.minimum(i, nc - 1))),
            pl.BlockSpec((f, TILE), lambda i: (0, jnp.where(i < nc, i, jnp.minimum(i - nc, nc - 1)))),
            pl.BlockSpec((m, TILE), lambda i: (0, jnp.minimum(late(i), nc - 1))),
            pl.BlockSpec((m, TILE), lambda i: (0, jnp.maximum(late(i) - nc, 0))),
        ],
        out_specs=pl.BlockSpec(memory_space=pl.ANY),
        out_shape=jax.ShapeDtypeStruct((2 * m, d), jnp.bfloat16),
        scratch_shapes=[
            pltpu.VMEM((2, nt, m // 2, TILE), jnp.float32),
            pltpu.VMEM((RING, m, TILE), jnp.float32),
            pltpu.VMEM((RING, m // 2, TILE), jnp.bfloat16),
            pltpu.VMEM((m, f), jnp.bfloat16),
            pltpu.SemaphoreType.DMA((2, nt)),
            pltpu.SemaphoreType.DMA((2, nt)),
            pltpu.SemaphoreType.DMA((2, nt)),
            pltpu.SemaphoreType.DMA((2, nt)),
            pltpu.SemaphoreType.DMA((nt,)),
        ],
        cost_estimate=pl.CostEstimate(flops=8 * m * f * d, bytes_accessed=6 * f * d + 12 * m * d, transcendentals=m * f),
        compiler_params=pltpu.CompilerParams(
            collective_id=0, has_side_effects=True, vmem_limit_bytes=67043328, dimension_semantics=("arbitrary",)),
        name="mlp_out",
    )(hid, u, w1, w3, w2, *xs)


def solution(mesh):
    sp = mesh.shape["sp"]
    nrep = mesh.shape["rep"]
    tok = P(("rep", "sp"), None)
    col = P(None, "tp")
    row = P("tp", None)
    cache = P("rep", ("tp", "sp"), None)

    def local(x, pos, g1, g2, wq, wk, wv, wo, w1, w3, w2):
        m, _ = x.shape
        n = m * sp
        ht = wq.shape[1] // HEAD_DIM
        kt = wk.shape[1] // HEAD_DIM
        qh = ht // sp
        t = lax.axis_index("tp")
        part = wo.shape[0] // (nrep * sp)
        mine = lax.axis_index("rep") * sp + lax.axis_index("sp")
        wo_all = lax.all_gather(lax.dynamic_slice_in_dim(wo, mine * part, part, 0), ("tp", "rep", "sp"), axis=0, tiled=True)

        u = _rms(x, g1)
        cs = _angles(pos)
        q = _rope(jnp.dot(u, wq, preferred_element_type=jnp.float32).reshape(m, ht, HEAD_DIM), cs).astype(jnp.bfloat16)
        k = _rope(jnp.dot(u, wk, preferred_element_type=jnp.float32).reshape(m, kt, HEAD_DIM), cs).astype(jnp.bfloat16)
        v = jnp.dot(u, wv, preferred_element_type=jnp.float32).astype(jnp.bfloat16).reshape(m, kt, HEAD_DIM)
        buf = jnp.concatenate([q.reshape(m, sp, qh, HEAD_DIM), k.reshape(m, sp, 1, HEAD_DIM), v.reshape(m, sp, 1, HEAD_DIM)], axis=2)
        buf = lax.all_to_all(buf.transpose(1, 2, 0, 3), "sp", 0, 0, tiled=True)
        ka = buf[:, qh].reshape(n, 1, HEAD_DIM)
        va = buf[:, qh + 1].reshape(n, 1, HEAD_DIM)
        att = _attention(buf, qh)
        att = lax.all_to_all(att, "sp", 0, 0, tiled=True)
        att = att.transpose(1, 0, 2).reshape(m, ht * HEAD_DIM)
        mc = m // 2
        a0, a1 = att[:mc], att[mc:]
        hops = [(a0, a0)]
        for k in range(1, 4):
            hops.append(_hop(*hops[-1], k))
        first = _side_by_side(a0, *zip(*hops[1:]), t)
        first, a1 = lax.optimization_barrier((first, a1))

        def mix(a, xr, g):
            o = jnp.dot(a, wo_all, preferred_element_type=jnp.float32)
            x1 = (xr.astype(jnp.float32) + o).astype(jnp.bfloat16)
            return x1, _rms(x1, g)

        hop1 = _hop(a1, a1, 1)
        x0, u0 = mix(first, x[:mc], g2)
        u0, hop1 = lax.optimization_barrier((u0, hop1))
        hop2 = _hop(*hop1, 2)
        h1 = jnp.dot(u0, w1, preferred_element_type=jnp.float32)
        u0, h1, hop2 = lax.optimization_barrier((u0, h1, hop2))
        hop3 = _hop(*hop2, 3)
        h3 = jnp.dot(u0, w3, preferred_element_type=jnp.float32)
        hid = (jax.nn.silu(h1) * h3).astype(jnp.bfloat16)
        hid, hop3, gb = lax.optimization_barrier((hid, hop3, g2))
        second = _side_by_side(a1, *zip(hop1, hop2, hop3), t)
        x1, u1 = mix(second, x[mc:], gb)
        y = _mlp_out(hid, u1, w1, w3, w2, (x0, x1))
        return y, ka, va

    return jax.shard_map(
        local,
        mesh=mesh,
        in_specs=(tok, P(("rep", "sp")), P(), P(), col, col, col, row, col, col, row),
        out_specs=(tok, cache, cache),
        check_vma=False,
    )
```

```python
import functools

import jax
import jax.numpy as jnp
from jax import lax
from jax.experimental import pallas as pl
from jax.experimental.pallas import tpu as pltpu
from jax.sharding import PartitionSpec as P


HEAD_DIM = 128
EPS = 1e-5
ROPE_BASE = 5e5
NEG = -1e30
QB = 512
KB = 512
TILE = 256
LAG = 2
RING = 3 * LAG + 2
MROWS = 256
MESH = pl.DeviceIdType.MESH


def _rms(x, g):
    x32 = x.astype(jnp.float32)
    r = lax.rsqrt(jnp.mean(x32 * x32, axis=-1, keepdims=True) + EPS)
    return (x32 * r * g).astype(jnp.bfloat16)


def _angles(pos):
    half = HEAD_DIM // 2
    inv = ROPE_BASE ** (-2.0 * jnp.arange(half, dtype=jnp.float32) / HEAD_DIM)
    ang = pos.astype(jnp.float32)[..., None] * inv
    return jnp.cos(ang)[..., None, :], jnp.sin(ang)[..., None, :]


def _rope(t, cs):
    c, s = cs
    half = HEAD_DIM // 2
    t1, t2 = t[..., :half], t[..., half:]
    return jnp.concatenate([t1 * c - t2 * s, t2 * c + t1 * s], axis=-1)


def _attn_kernel(q_ref, k_ref, v_ref, o_ref, *, heads, per_src, c):
    i = pl.program_id(0) * per_src + c
    scale = HEAD_DIM ** -0.5
    q = q_ref[0].reshape(heads * QB, HEAD_DIM)
    rows = heads * QB

    def scores(j):
        kb = k_ref[j // per_src, 0, pl.ds((j % per_src) * KB, KB), :]
        return lax.dot_general(q, kb, (((1,), (1,)), ((), ())), preferred_element_type=jnp.float32) * scale

    def update(j, s, carry):
        m, l, acc = carry
        mn = jnp.maximum(m, jnp.max(s, axis=1, keepdims=True))
        a = jnp.exp(m - mn)
        p = jnp.exp(s - mn)
        l = l * a + jnp.sum(p, axis=1, keepdims=True)
        vb = v_ref[j // per_src, 0, pl.ds((j % per_src) * KB, KB), :]
        acc = acc * a + jnp.dot(p.astype(jnp.bfloat16), vb, preferred_element_type=jnp.float32)
        return mn, l, acc

    init = (
        jnp.full((rows, 1), NEG, jnp.float32),
        jnp.zeros((rows, 1), jnp.float32),
        jnp.zeros((rows, HEAD_DIM), jnp.float32),
    )
    carry = lax.fori_loop(0, i, lambda j, c: update(j, scores(j), c), init)
    r = lax.broadcasted_iota(jnp.int32, (heads, QB, KB), 1)
    c = lax.broadcasted_iota(jnp.int32, (heads, QB, KB), 2)
    s = jnp.where((r >= c).reshape(rows, KB), scores(i), NEG)
    _, l, acc = update(i, s, carry)
    o = (acc / l).astype(jnp.bfloat16)
    for h in range(heads):
        o_ref[0, :, h * HEAD_DIM:(h + 1) * HEAD_DIM] = o[h * QB:(h + 1) * QB]


def _attention(buf, heads, c):
    sp, _, m, dh = buf.shape
    per = m // QB
    n = sp * m
    return pl.pallas_call(
        functools.partial(_attn_kernel, heads=heads, per_src=per, c=c),
        grid=(sp,),
        in_specs=[
            pl.BlockSpec((1, heads, QB, dh), lambda i: (i, 0, c, 0)),
            pl.BlockSpec((sp, 1, m, dh), lambda i: (0, heads, 0, 0)),
            pl.BlockSpec((sp, 1, m, dh), lambda i: (0, heads + 1, 0, 0)),
        ],
        out_specs=pl.BlockSpec((1, QB, heads * dh), lambda i: (i, 0, 0)),
        out_shape=jax.ShapeDtypeStruct((sp, QB, heads * dh), jnp.bfloat16),
        cost_estimate=pl.CostEstimate(flops=heads * n * n * dh, bytes_accessed=8 * n * dh * 2, transcendentals=heads * n * n // 4),
        compiler_params=pltpu.CompilerParams(vmem_limit_bytes=48 * 1024 * 1024),
        name="attn",
    )(buf, buf, buf)


def _hop(up, dn, k):
    up = lax.ppermute(up, "tp", [(i, i + 1) for i in range(k - 1, 3)])
    dn = lax.ppermute(dn, "tp", [(i, i - 1) for i in range(1, 5 - k)])
    return up, dn


def _side_by_side(a, up, dn, t):
    out = []
    for s in range(4):
        b = a
        for d in range(4):
            if d < s:
                b = jnp.where(t == d, dn[s - d - 1], b)
            elif d > s:
                b = jnp.where(t == d, up[d - s - 1], b)
        out.append(b)
    return jnp.concatenate(out, axis=1)


def _mlp_kernel(hid_ref, u_ref, w1_ref, w3_ref, w2_ref, x0_ref, x1_ref, y_ref, acc, part, fin, hid, sf, rf, sb, rb, sl, *, nc, nt):
    i = pl.program_id(0)
    t = lax.axis_index("tp")
    m = part.shape[1]
    h = m // 2

    @pl.when(i == 0)
    def _():
        barrier = pltpu.get_barrier_semaphore()

        @pl.when(t > 0)
        def _():
            pl.semaphore_signal(barrier, inc=1, device_id={"tp": t - 1}, device_id_type=MESH)

        @pl.when(t < 3)
        def _():
            pl.semaphore_signal(barrier, inc=1, device_id={"tp": t + 1}, device_id_type=MESH)

        pl.semaphore_wait(barrier, jnp.where((t == 0) | (t == 3), 1, 2))

    def place(s, g):
        row = pl.multiple_of((g // nc) * m + s * h, h)
        return y_ref.at[pl.ds(row, h), pl.ds(pl.multiple_of((g % nc) * TILE, TILE), TILE)]

    def forward(s, g, dev):
        return pltpu.make_async_remote_copy(
            src_ref=acc.at[s, g], dst_ref=acc.at[s, g], send_sem=sf.at[s, g], recv_sem=rf.at[s, g],
            device_id={"tp": dev}, device_id_type=MESH)

    def back(s, g, dev, src):
        return pltpu.make_async_remote_copy(
            src_ref=src, dst_ref=place(s, g), send_sem=sb.at[s, g], recv_sem=rb.at[s, g],
            device_id={"tp": dev}, device_id_type=MESH)

    def keep(s, g):
        return pltpu.make_async_copy(fin.at[g % RING], place(s, g), sl.at[g])

    def settle(s, g, dev):
        back(s, g, dev, fin.at[g % RING]).wait_send()
        keep(s, g).wait()

    other = jnp.where(t < 2, t + 1, t - 1)
    for s in range(2):
        pos = 3 - t if s == 0 else t
        nxt = t - 1 if s == 0 else t + 1
        prv = t + 1 if s == 0 else t - 1
        rows = slice(s * h, (s + 1) * h)
        g = i - 1 - pos * LAG
        on = (g >= 0) & (g < nt)

        @pl.when(on & (pos == 0))
        def _():
            acc[s, g] = part[g % RING, rows, :]
            forward(s, g, nxt).start()

        @pl.when(on & (pos > 0) & (pos < 3))
        def _():
            forward(s, g, other).wait_recv()
            acc[s, g] = acc[s, g] + part[g % RING, rows, :]
            forward(s, g, nxt).start()

        @pl.when(on & (pos == 3))
        def _():
            forward(s, g, other).wait_recv()
            total = acc[s, g] + part[g % RING, rows, :]

            @pl.when(g >= RING)
            def _():
                settle(s, g - RING, prv)

            res = jnp.where(g < nc, x0_ref[rows, :].astype(jnp.float32), x1_ref[rows, :].astype(jnp.float32))
            fin[g % RING] = (res + total).astype(jnp.bfloat16)
            back(s, g, prv, fin.at[g % RING]).start()
            keep(s, g).start()

        gb = i - 1 - 3 * LAG - (3 - pos) * LAG
        onb = (gb >= 0) & (gb < nt)

        @pl.when(onb & (pos > 0) & (pos < 3))
        def _():
            back(s, gb, other, place(s, gb)).wait_recv()
            back(s, gb, prv, place(s, gb)).start()

        @pl.when(onb & (pos == 0))
        def _():
            back(s, gb, other, place(s, gb)).wait_recv()

    def blocks(body):
        def step(b, _):
            body(pl.ds(pl.multiple_of(b * MROWS, MROWS), MROWS))
            return 0

        lax.fori_loop(0, m // MROWS, step, 0)

    @pl.when(i < nc)
    def _():
        cols = pl.ds(pl.multiple_of(i * TILE, TILE), TILE)

        def body(r):
            a = jnp.dot(u_ref[r, :], w1_ref[...], preferred_element_type=jnp.float32)
            b = jnp.dot(u_ref[r, :], w3_ref[...], preferred_element_type=jnp.float32)
            hid[r, cols] = (jax.nn.silu(a) * b).astype(jnp.bfloat16)
            part[i % RING, r, :] = jnp.dot(hid_ref[r, :], w2_ref[...], preferred_element_type=jnp.float32)

        blocks(body)

    @pl.when((i >= nc) & (i < nt))
    def _():
        def body(r):
            part[i % RING, r, :] = jnp.dot(hid[r, :], w2_ref[...], preferred_element_type=jnp.float32)

        blocks(body)

    @pl.when(i == nt + 6 * LAG)
    def _():
        for s in range(2):
            pos = 3 - t if s == 0 else t

            def drain(g, _):
                @pl.when(pos < 3)
                def _():
                    forward(s, g, other).wait_send()

                @pl.when((pos > 0) & (pos < 3))
                def _():
                    back(s, g, other, place(s, g)).wait_send()

                @pl.when((pos == 3) & (g >= nt - RING))
                def _():
                    settle(s, g, other)

                return 0

            lax.fori_loop(0, nt, drain, 0)


def _mlp_out(hid, u, w1, w3, w2, xs):
    m, f = hid.shape
    d = w2.shape[1]
    nc = d // TILE
    nt = 2 * nc
    assert f == d

    def late(i):
        return jnp.clip(i - 1 - 3 * LAG, 0, nt - 1)

    once = pl.Buffered(1)
    return pl.pallas_call(
        functools.partial(_mlp_kernel, nc=nc, nt=nt),
        grid=(nt + 6 * LAG + 1,),
        in_specs=[
            pl.BlockSpec((m, f), lambda i: (0, 0), pipeline_mode=once),
            pl.BlockSpec((m, u.shape[1]), lambda i: (0, 0), pipeline_mode=once),
            pl.BlockSpec((w1.shape[0], TILE), lambda i: (0, jnp.minimum(i, nc - 1))),
            pl.BlockSpec((w3.shape[0], TILE), lambda i: (0, jnp.minimum(i, nc - 1))),
            pl.BlockSpec((f, TILE), lambda i: (0, jnp.where(i < nc, i, jnp.minimum(i - nc, nc - 1)))),
            pl.BlockSpec((m, TILE), lambda i: (0, jnp.minimum(late(i), nc - 1))),
            pl.BlockSpec((m, TILE), lambda i: (0, jnp.maximum(late(i) - nc, 0))),
        ],
        out_specs=pl.BlockSpec(memory_space=pl.ANY),
        out_shape=jax.ShapeDtypeStruct((2 * m, d), jnp.bfloat16),
        scratch_shapes=[
            pltpu.VMEM((2, nt, m // 2, TILE), jnp.float32),
            pltpu.VMEM((RING, m, TILE), jnp.float32),
            pltpu.VMEM((RING, m // 2, TILE), jnp.bfloat16),
            pltpu.VMEM((m, f), jnp.bfloat16),
            pltpu.SemaphoreType.DMA((2, nt)),
            pltpu.SemaphoreType.DMA((2, nt)),
            pltpu.SemaphoreType.DMA((2, nt)),
            pltpu.SemaphoreType.DMA((2, nt)),
            pltpu.SemaphoreType.DMA((nt,)),
        ],
        cost_estimate=pl.CostEstimate(flops=8 * m * f * d, bytes_accessed=6 * f * d + 12 * m * d, transcendentals=m * f),
        compiler_params=pltpu.CompilerParams(
            collective_id=0, has_side_effects=True, vmem_limit_bytes=67043328, dimension_semantics=("arbitrary",)),
        name="mlp_out",
    )(hid, u, w1, w3, w2, *xs)


def solution(mesh):
    sp = mesh.shape["sp"]
    nrep = mesh.shape["rep"]
    tok = P(("rep", "sp"), None)
    col = P(None, "tp")
    row = P("tp", None)
    cache = P("rep", ("tp", "sp"), None)

    def local(x, pos, g1, g2, wq, wk, wv, wo, w1, w3, w2):
        m, _ = x.shape
        n = m * sp
        ht = wq.shape[1] // HEAD_DIM
        kt = wk.shape[1] // HEAD_DIM
        qh = ht // sp
        t = lax.axis_index("tp")
        part = wo.shape[0] // (nrep * sp)
        mine = lax.axis_index("rep") * sp + lax.axis_index("sp")
        wo_all = lax.all_gather(lax.dynamic_slice_in_dim(wo, mine * part, part, 0), ("tp", "rep", "sp"), axis=0, tiled=True)

        u = _rms(x, g1)
        cs = _angles(pos)
        q = _rope(jnp.dot(u, wq, preferred_element_type=jnp.float32).reshape(m, ht, HEAD_DIM), cs).astype(jnp.bfloat16)
        k = _rope(jnp.dot(u, wk, preferred_element_type=jnp.float32).reshape(m, kt, HEAD_DIM), cs).astype(jnp.bfloat16)
        v = jnp.dot(u, wv, preferred_element_type=jnp.float32).astype(jnp.bfloat16).reshape(m, kt, HEAD_DIM)
        buf = jnp.concatenate([q.reshape(m, sp, qh, HEAD_DIM), k.reshape(m, sp, 1, HEAD_DIM), v.reshape(m, sp, 1, HEAD_DIM)], axis=2)
        buf = lax.all_to_all(buf.transpose(1, 2, 0, 3), "sp", 0, 0, tiled=True)
        ka = buf[:, qh].reshape(n, 1, HEAD_DIM)
        va = buf[:, qh + 1].reshape(n, 1, HEAD_DIM)
        mc = m // 2

        def rows(b, c):
            a = lax.all_to_all(_attention(b, qh, c), "sp", 0, 0, tiled=True)
            return a.transpose(1, 0, 2).reshape(mc, ht * HEAD_DIM)

        a0, buf = lax.optimization_barrier((rows(buf, 0), buf))
        hops = [(a0, a0), _hop(a0, a0, 1)]
        a1 = rows(buf, 1)
        a1, hops[1] = lax.optimization_barrier((a1, hops[1]))
        for k in range(2, 4):
            hops.append(_hop(*hops[-1], k))
        first = _side_by_side(a0, *zip(*hops[1:]), t)
        first, a1 = lax.optimization_barrier((first, a1))

        def mix(a, xr, g):
            o = jnp.dot(a, wo_all, preferred_element_type=jnp.float32)
            x1 = (xr.astype(jnp.float32) + o).astype(jnp.bfloat16)
            return x1, _rms(x1, g)

        hop1 = _hop(a1, a1, 1)
        x0, u0 = mix(first, x[:mc], g2)
        u0, hop1 = lax.optimization_barrier((u0, hop1))
        hop2 = _hop(*hop1, 2)
        h1 = jnp.dot(u0, w1, preferred_element_type=jnp.float32)
        u0, h1, hop2 = lax.optimization_barrier((u0, h1, hop2))
        hop3 = _hop(*hop2, 3)
        h3 = jnp.dot(u0, w3, preferred_element_type=jnp.float32)
        hid = (jax.nn.silu(h1) * h3).astype(jnp.bfloat16)
        hid, hop3, gb = lax.optimization_barrier((hid, hop3, g2))
        second = _side_by_side(a1, *zip(hop1, hop2, hop3), t)
        x1, u1 = mix(second, x[mc:], gb)
        y = _mlp_out(hid, u1, w1, w3, w2, (x0, x1))
        return y, ka, va

    return jax.shard_map(
        local,
        mesh=mesh,
        in_specs=(tok, P(("rep", "sp")), P(), P(), col, col, col, row, col, col, row),
        out_specs=(tok, cache, cache),
        check_vma=False,
    )
```
